32 devices in a mesh: pipe: 2 (over x), tensor: 2 (over core), dp: 8 (over z, y).
Axes of the slice: x: 2, y: 2, z: 4, core: 2. Of those that a mesh axis runs over, the one named last changes fastest.
Arguments:
- attn_out: bfloat16 [2, 4, 1024, 4096], P('pipe', None, 'dp', 'tensor'), may hold values from -6 to 6
- grad_top: bfloat16 [4, 1024, 4096], P(None, 'dp', 'tensor'), may hold values from -6 to 6
- branch_grad: bfloat16 [2, 4, 1024, 4096], P('pipe', None, 'dp', 'tensor'), may hold values from -6 to 6
- error_prev: bfloat16 [2, 8, 4096, 4096], P('pipe', 'dp', 'tensor'), may hold values from -0.3984375 to 0.3984375
- q_prev: float32 [2, 4096, 64], P('pipe', 'tensor'), may hold values from -6 to 6
Outputs:
- grad_input: bfloat16 [2, 4, 1024, 4096], P('pipe', None, 'dp', 'tensor')
- error_next: bfloat16 [2, 8, 4096, 4096], P('pipe', 'dp', 'tensor')
- p_factor: float32 [2, 4096, 64], P('pipe', 'tensor')
- q_factor: float32 [2, 4096, 64], P('pipe', 'tensor')
The draws below stay inside these ranges and needn't reach their ends.
All inputs are finite; a program needn't handle non-finite values.
Results may differ from the reference program's by a relative error of at most 0.012.
Values may be sent and summed in bfloat16 or wider, within the bound.
A program may use at most 256 MiB of HBM per device.

```python
import jax
import jax.numpy as jnp
from jax import lax

D = 4096
RANK = 64
MB = 4
TOK_MB = 128
TOKS = 1024
HDALL = 4096
N_PIPE = 2
N_DP = 8


def shard_levels(stream_key, extent, shards, smallest, top_value):
    factor_of = 1.0
    for position, parts in shards:
        heights = jax.random.uniform(jax.random.fold_in(jax.random.fold_in(stream_key, 6), position), (parts,), jnp.float32, smallest / len(shards), top_value / len(shards))
        factor_of = factor_of * jnp.repeat(jnp.exp(heights), extent[position] // parts).reshape((-1,) + (1,) * (len(extent) - 1 - position))
    return factor_of


def noise(rng, shape, deviation, bound, pieces=(), held_as=jnp.bfloat16):
    drawn = deviation * jax.random.normal(rng, shape, jnp.float32)
    if pieces:
        drawn = drawn * shard_levels(rng, shape, pieces, -0.22, 0.18)
    return jnp.clip(drawn, -bound, bound).astype(held_as)


def setup_inputs(seed: int = 0) -> dict:
    splits = jax.random.split(jax.random.key(seed), 6)
    return {
        "attn_out": noise(splits[0], (N_PIPE, MB, TOKS, HDALL), 1.0, 6.0, ((0, 2), (2, 8), (3, 2))),
        "grad_top": noise(splits[1], (MB, TOKS, D), 1.0, 6.0, ((1, 8), (2, 2))),
        "branch_grad": noise(splits[2], (N_PIPE, MB, TOKS, D), 1.0, 6.0, ((0, 2), (2, 8), (3, 2))),
        "error_prev": noise(splits[3], (N_PIPE, N_DP, HDALL, D), 0.05, 0.3984375, ((0, 2), (1, 8), (2, 2))),
        "q_prev": noise(splits[4], (N_PIPE, D, RANK), 1.0, 6.0, ((0, 2), (1, 2)), jnp.float32),
    }


def orthonormal(praw):
    gram = jnp.dot(praw.T, praw, precision=lax.Precision.HIGHEST)
    lower = jnp.linalg.cholesky(gram)
    return lax.linalg.triangular_solve(lower, praw, left_side=False, lower=True, transpose_a=True)

def reference(attn_out, grad_top, branch_grad, error_prev, q_prev):
    scale = 1.0 / (MB * TOK_MB)
    high = lax.Precision.HIGHEST
    out_grad = grad_top
    inputs, errors, pfacts, qfacts = ([], [], [], [])
    for section in reversed(range(N_PIPE)):
        grad_in = (out_grad.astype(jnp.float32) + branch_grad[section].astype(jnp.float32)).astype(jnp.bfloat16)
        acts = attn_out[section].reshape(MB, N_DP, TOK_MB, HDALL).transpose(1, 0, 2, 3)
        grads = out_grad.reshape(MB, N_DP, TOK_MB, D).transpose(1, 0, 2, 3)

        def local(triple):
            act_rep, grad_rep, err_rep = triple
            total = jnp.zeros((HDALL, D), jnp.float32)
            for micro in range(MB):
                total = total + jnp.dot(act_rep[micro].T.astype(jnp.float32), grad_rep[micro].astype(jnp.float32), preferred_element_type=jnp.float32)
            return total * scale + err_rep.astype(jnp.float32)
        mats = lax.map(local, (acts, grads, error_prev[section]))
        qold = q_prev[section]
        praw = jnp.sum(lax.map(lambda mat: jnp.dot(mat, qold, precision=high), mats), axis=0) / N_DP
        phat = orthonormal(praw)
        qnew = jnp.sum(lax.map(lambda mat: jnp.dot(mat.T, phat, precision=high), mats), axis=0) / N_DP
        err = lax.map(lambda mat: (mat - jnp.dot(phat, qnew.T, precision=high)).astype(jnp.bfloat16), mats)
        inputs.insert(0, grad_in)
        errors.insert(0, err)
        pfacts.insert(0, phat)
        qfacts.insert(0, qnew)
        out_grad = grad_in
    return (jnp.stack(inputs), jnp.stack(errors), jnp.stack(pfacts), jnp.stack(qfacts))
```

```python
import jax
import jax.numpy as jnp
from jax import lax
from jax.sharding import PartitionSpec as P


def from_behind(value, axis, by):
    devices = lax.axis_size(axis)
    pairs = [(i, i + by) for i in range(devices) if 0 <= i + by < devices]
    return lax.ppermute(value, axis, pairs)


def add_round(a, b):
    return (a.astype(jnp.float32) + b.astype(jnp.float32)).astype(jnp.bfloat16)


def two_terms(x):
    head = x.astype(jnp.bfloat16)
    tail = (x - head.astype(jnp.float32)).astype(jnp.bfloat16)
    return head, tail


def sum_of_shares(value, axes):
    count = lax.axis_size(axes)
    rows, cols = value.shape
    pieces = value.astype(jnp.bfloat16).reshape(count, rows // count, cols)
    landed = lax.all_to_all(pieces, axes, split_axis=0, concat_axis=0, tiled=True)
    return jnp.sum(landed.astype(jnp.float32), axis=0)


def on_device(attn_out, grad_top, branch_grad, error_prev, q_prev):
    high = lax.Precision.HIGHEST
    section = lax.axis_index("pipe")
    sections = lax.axis_size("pipe")
    last = sections - 1
    micro_count, tok_rows, features = grad_top.shape
    head_rows = attn_out.shape[3]
    replicas = lax.axis_size("dp")
    tokens = micro_count * tok_rows
    branch = branch_grad[0]

    out_grads, grad_ins = [], []
    for micro in range(micro_count):
        out = grad_top[micro]
        for hop in range(sections - 1):
            if hop == 0:
                back = add_round(grad_top[micro], from_behind(branch[micro], "pipe", -1))
            else:
                back = from_behind(add_round(out, branch[micro]), "pipe", -1)
            out = jnp.where(section == last, grad_top[micro], back)
        out_grads.append(out)
        grad_ins.append(add_round(out, branch[micro]))
    grad_all = jnp.stack(grad_ins)
    out_all = lax.all_gather(jnp.concatenate(out_grads, axis=0), "tensor", axis=1, tiled=True)
    grads = lax.dot_general(
        attn_out[0].reshape(tokens, head_rows),
        out_all,
        (((0,), (0,)), ((), ())),
        preferred_element_type=jnp.float32,
    )
    matrix = (grads / tokens + error_prev[0, 0].astype(jnp.float32)).astype(jnp.bfloat16)

    rank = q_prev.shape[2]
    q_old = lax.all_gather(q_prev[0], "tensor", axis=0, tiled=True)
    p_two = jnp.dot(
        matrix, jnp.concatenate(two_terms(q_old), axis=1), preferred_element_type=jnp.float32
    )
    p_local = p_two[:, :rank] + p_two[:, rank:]
    p_rows = sum_of_shares(p_local, "dp") / replicas
    praw = lax.all_gather(p_rows, "dp", axis=0, tiled=True)
    gram = lax.psum(jnp.dot(praw.T, praw, precision=high), "tensor")
    lower = jnp.linalg.cholesky(gram)
    phat = lax.linalg.triangular_solve(lower, praw, left_side=False, lower=True, transpose_a=True)
    p_terms = jnp.concatenate(two_terms(phat), axis=1)
    q_two = lax.dot_general(
        matrix, p_terms, (((0,), (0,)), ((), ())), preferred_element_type=jnp.float32
    )
    q_local = q_two[:, :rank] + q_two[:, rank:]
    q_rows = sum_of_shares(q_local, ("tensor", "dp")) / replicas
    q_full = lax.all_gather(q_rows.astype(jnp.bfloat16), ("tensor", "dp"), axis=0, tiled=True)
    own = q_prev.shape[1]
    q_own = lax.dynamic_slice_in_dim(q_full, lax.axis_index("tensor") * own, own, 0)
    low_rank = lax.dot_general(
        p_terms,
        jnp.concatenate([q_full, q_full], axis=1),
        (((1,), (1,)), ((), ())),
        preferred_element_type=jnp.float32,
    )
    error_next = (matrix.astype(jnp.float32) - low_rank).astype(jnp.bfloat16)
    return (grad_all[None], error_next[None, None], phat[None], q_own.astype(jnp.float32)[None])


def solution(mesh):
    return jax.shard_map(
        on_device,
        mesh=mesh,
        in_specs=(
            P("pipe", None, "dp", "tensor"),
            P(None, "dp", "tensor"),
            P("pipe", None, "dp", "tensor"),
            P("pipe", "dp", "tensor", None),
            P("pipe", "tensor", None),
        ),
        out_specs=(
            P("pipe", None, "dp", "tensor"),
            P("pipe", "dp", "tensor", None),
            P("pipe", "tensor", None),
            P("pipe", "tensor", None),
        ),
        check_vma=False,
    )
```
